256 devices in a mesh: rep: 32 (over z, y), data: 8 (over x, core).
Axes of the slice: x: 4, y: 4, z: 8, core: 2. Of those that a mesh axis runs over, the one named last changes fastest.
Arguments:
- img_feat: bfloat16 [196608, 1024], P(('rep', 'data'))
- txt_feat: bfloat16 [196608, 1024], P(('rep', 'data'))
- w_img: bfloat16 [1024, 1024], replicated
- w_txt: bfloat16 [1024, 1024], replicated
- log_temp: float32 [], replicated
- logit_bias: float32 [], replicated
Outputs:
- output 1: float32 [], replicated
- output 2: float32 [], replicated
- output 3: float32 [], replicated
- output 4: float32 [1024, 1024], replicated
- output 5: float32 [1024, 1024], replicated
All inputs are finite; a program needn't handle non-finite values.
Results may differ from the reference program's by a relative error of at most 0.001.
Values are sent between devices in bfloat16 or wider.
A program may use at most 768 MiB of HBM per device.

```python
import math
import jax
import jax.numpy as jnp
from jax import lax

FI = 1024
FT = 1024
D = 1024
BLOCK_ROWS = 768
BLOCKS = 8
GROUPS = 32
LATENT = 16
GROUP_ROWS = BLOCK_ROWS * BLOCKS
TOTAL_ROWS = GROUP_ROWS * GROUPS


def draw_features(mean_key, shift_key, mix_key, noise_key, latent, width):
    feat_mean = jax.random.normal(mean_key, (width,), jnp.float32)
    block_shift = jnp.repeat(jax.random.normal(shift_key, (BLOCKS * GROUPS, width), jnp.float32), BLOCK_ROWS, axis=0)
    latent_mix = jax.random.normal(mix_key, (LATENT, width), jnp.float32) * LATENT ** -0.5
    noise_rows = jax.random.normal(noise_key, (TOTAL_ROWS, width), jnp.float32)
    features = feat_mean[None, :] + 0.6 * block_shift + 0.8 * jnp.dot(latent, latent_mix) + 0.5 * noise_rows
    return features.astype(jnp.bfloat16)


def setup_inputs(seed: int = 0) -> dict:
    root_key = jax.random.key(seed)
    sub_keys = jax.random.split(root_key, 13)
    latent = jax.random.normal(sub_keys[0], (TOTAL_ROWS, LATENT), jnp.float32)
    img_feat = draw_features(sub_keys[1], sub_keys[2], sub_keys[3], sub_keys[4], latent, FI)
    txt_feat = draw_features(sub_keys[5], sub_keys[6], sub_keys[7], sub_keys[8], latent, FT)
    w_img = (jax.random.normal(sub_keys[9], (FI, D), jnp.float32) * FI ** -0.5).astype(jnp.bfloat16)
    w_txt = (jax.random.normal(sub_keys[10], (FT, D), jnp.float32) * FT ** -0.5).astype(jnp.bfloat16)
    log_temp = (math.log(5.0) + 0.3 * jax.random.normal(sub_keys[11], (), jnp.float32)).astype(jnp.float32)
    logit_bias = (0.5 * jax.random.normal(sub_keys[12], (), jnp.float32) - math.log(GROUP_ROWS)).astype(jnp.float32)
    return {"img_feat": img_feat, "txt_feat": txt_feat, "w_img": w_img, "w_txt": w_txt, "log_temp": log_temp, "logit_bias": logit_bias}


def normalize_rows(raw_emb):
    inv_norm = lax.rsqrt(jnp.sum(raw_emb * raw_emb, axis=1, keepdims=True))
    return raw_emb * inv_norm, inv_norm


def backward_norm(grad_unit, unit_emb, inv_norm):
    proj = jnp.sum(unit_emb * grad_unit, axis=1, keepdims=True)
    return (inv_norm * (grad_unit - unit_emb * proj)).astype(jnp.bfloat16)


def group_terms(img_grp, txt_grp, temp_scale, logit_bias):
    img_blocks = img_grp.reshape(BLOCKS, BLOCK_ROWS, D)
    col_ids = jnp.arange(GROUP_ROWS)[None, :]

    def block_step(loop_state, block_in):
        txt_acc, scal_acc = loop_state
        img_blk, blk_idx = block_in
        row_ids = blk_idx * BLOCK_ROWS + jnp.arange(BLOCK_ROWS)[:, None]
        sign_mat = jnp.where(row_ids == col_ids, 1.0, -1.0)
        tile_dots = jnp.dot(img_blk, txt_grp.T, preferred_element_type=jnp.float32)
        logits = temp_scale * tile_dots + logit_bias
        margin = sign_mat * logits
        grad_z = -sign_mat * jax.nn.sigmoid(-margin) / TOTAL_ROWS
        scal_part = jnp.stack([jnp.sum(jax.nn.softplus(-margin)), temp_scale * jnp.sum(grad_z * tile_dots), jnp.sum(grad_z)])
        h_mat = (temp_scale * grad_z).astype(jnp.bfloat16)
        img_grad = jnp.dot(h_mat, txt_grp, preferred_element_type=jnp.float32)
        txt_acc = txt_acc + jnp.dot(h_mat.T, img_blk, preferred_element_type=jnp.float32)
        return (txt_acc, scal_acc + scal_part), img_grad

    init_state = (jnp.zeros((GROUP_ROWS, D), jnp.float32), jnp.zeros((3,), jnp.float32))
    final_state, img_grads = lax.scan(block_step, init_state, (img_blocks, jnp.arange(BLOCKS)))
    return img_grads.reshape(GROUP_ROWS, D), final_state[0], final_state[1]


def reference(img_feat, txt_feat, w_img, w_txt, log_temp, logit_bias):
    temp_scale = jnp.exp(log_temp)
    unit_img, inv_img = normalize_rows(jnp.dot(img_feat, w_img, preferred_element_type=jnp.float32))
    unit_txt, inv_txt = normalize_rows(jnp.dot(txt_feat, w_txt, preferred_element_type=jnp.float32))
    emb_img = unit_img.astype(jnp.bfloat16).reshape(GROUPS, GROUP_ROWS, D)
    emb_txt = unit_txt.astype(jnp.bfloat16).reshape(GROUPS, GROUP_ROWS, D)

    def per_group(group_embs):
        return group_terms(group_embs[0], group_embs[1], temp_scale, logit_bias)

    img_grad, txt_grad, scal_sums = lax.map(per_group, (emb_img, emb_txt))
    raw_img_grad = backward_norm(img_grad.reshape(TOTAL_ROWS, D), unit_img, inv_img)
    raw_txt_grad = backward_norm(txt_grad.reshape(TOTAL_ROWS, D), unit_txt, inv_txt)
    dw_img = jnp.dot(img_feat.T, raw_img_grad, preferred_element_type=jnp.float32)
    dw_txt = jnp.dot(txt_feat.T, raw_txt_grad, preferred_element_type=jnp.float32)
    scal_total = jnp.sum(scal_sums, axis=0)
    return scal_total[0] / TOTAL_ROWS, scal_total[1], scal_total[2], dw_img, dw_txt
```

```python
import functools

import jax
import jax.numpy as jnp
from jax import lax
from jax.experimental import pallas as pl
from jax.experimental.pallas import tpu as pltpu
from jax.sharding import PartitionSpec as P

F32 = jnp.float32
BF16 = jnp.bfloat16
MESH = pl.DeviceIdType.MESH
X_N, C_N, Y_N, Z_N = 4, 2, 4, 8
VMEM_CAP = 67_043_328


def greet(peers):
    barrier = pltpu.get_barrier_semaphore()
    for peer in peers:
        pl.semaphore_signal(barrier, inc=1, device_id=peer, device_id_type=MESH)
    pl.semaphore_wait(barrier, len(peers))


def remote(src, dst, send_sem, recv_sem, peer):
    return pltpu.make_async_remote_copy(
        src_ref=src, dst_ref=dst, send_sem=send_sem, recv_sem=recv_sem, device_id=peer, device_id_type=MESH
    )


def fold_sum(val):
    rows, cols = val.shape
    return jnp.sum(val.reshape(rows // 8, 8, cols), axis=0)


def fold_log1p(exps):
    rows, cols = exps.shape
    parts = exps.reshape(rows // 8, 8, cols)
    count = rows // 8
    while count > 1:
        if count % 2:
            low, high, tail = parts[: count // 2], parts[count // 2 : count - 1], parts[count - 1 :]
            merged = low + high + low * high
            first = merged[:1]
            first = first + tail + first * tail
            parts = first if count == 3 else jnp.concatenate([first, merged[1:]], axis=0)
        else:
            low, high = parts[: count // 2], parts[count // 2 :]
            parts = low + high + low * high
        count //= 2
    return jnp.log1p(parts[0])


def main_kernel(total_rows, rows, dim, sc_ref, img_ref, txt_ref, wi_ref, wt_ref, dw_ref, scal_ref,
                xq, xk, wq, wk, kbuf, eq, unit, inv, acc, sblk0, sblk1, hblk0, hblk1, sums,
                ld_sem, xs_sem, xr_sem, ks_sem, kr_sem):
    tile = rows // 3
    qt = rows // 2
    rep = lax.axis_index("rep")
    dat = lax.axis_index("data")
    x, c = dat // 2, dat % 2
    kind = x % 2
    step = 1 - 2 * c
    dst_x = (x + step + X_N) % X_N
    src_x = (x - step + X_N) % X_N
    partner = (rep, x * 2 + 1 - c)
    dst = (rep, dst_x * 2 + c)
    src = (rep, src_x * 2 + c)
    scale, bias = sc_ref[0], sc_ref[1]
    h_scale = scale * F32(1.0 / total_rows)
    sblk = (sblk0, sblk1)
    hblk = (hblk0, hblk1)

    def load(from_ref, to_ref, idx):
        return pltpu.make_async_copy(from_ref, to_ref, ld_sem.at[idx])

    own = pl.ds(0, rows)
    swp = pl.ds(rows, rows)

    @pl.when(kind == 0)
    def _():
        load(txt_ref, xk, 0).start()
        load(img_ref, xq.at[own], 1).start()
        load(wi_ref, wq, 2).start()
        load(wt_ref, wk, 3).start()

    @pl.when(kind == 1)
    def _():
        load(img_ref, xk, 0).start()
        load(txt_ref, xq.at[own], 1).start()
        load(wt_ref, wq, 2).start()
        load(wi_ref, wk, 3).start()

    greet((partner, dst, src))
    load(txt_ref, xk, 0).wait()
    swap_copy = remote(xk, xq.at[swp], xs_sem, xr_sem, dst)
    swap_copy.start()

    def krows(slot, t):
        return kbuf.at[slot, pl.ds(pl.multiple_of(t * tile, tile), tile)]

    def erows(base, t):
        return eq.at[pl.ds(pl.multiple_of(base + t * tile, tile), tile)]

    def own_to_dst(t):
        return remote(erows(0, t), krows(4, t), ks_sem.at[0, t], kr_sem.at[4, t], dst)

    def own_to_src(t):
        return remote(erows(0, t), krows(2, t), ks_sem.at[1, t], kr_sem.at[2, t], src)

    def swp_to_dst(t):
        return remote(erows(rows, t), krows(6, t), ks_sem.at[2, t], kr_sem.at[6, t], dst)

    def to_partner(slot, t):
        return remote(krows(slot, t), krows(slot + 1, t), ks_sem.at[3 + slot // 2, t], kr_sem.at[slot + 1, t], partner)

    def got(slot, t):
        remote(krows(slot, t), krows(slot, t), ks_sem.at[0, t], kr_sem.at[slot, t], partner).wait_recv()

    def project_q(base, t):
        at = pl.ds(pl.multiple_of(base + t * tile, tile), tile)
        raw = jnp.dot(xq[at], wq[...], preferred_element_type=F32)
        inv_norm = lax.rsqrt(jnp.sum(raw * raw, axis=1, keepdims=True))
        val = raw * inv_norm
        unit[at] = val
        eq[at] = val.astype(BF16)
        inv[at] = jnp.broadcast_to(inv_norm, (tile, 128))

    def project_k(t):
        at = pl.ds(pl.multiple_of(t * tile, tile), tile)
        raw = jnp.dot(xk[at], wk[...], preferred_element_type=F32)
        inv_norm = lax.rsqrt(jnp.sum(raw * raw, axis=1, keepdims=True))
        kbuf[0, at] = (raw * inv_norm).astype(BF16)

    def send_own(t):
        own_to_src(t).start()
        own_to_dst(t).start()

    load(img_ref, xq.at[own], 1).wait()
    load(wi_ref, wq, 2).wait()

    def own_step(t, carry):
        project_q(0, t)

        @pl.when(t > 0)
        def _():
            send_own(t - 1)

        return carry

    lax.fori_loop(0, 3, own_step, 0)
    load(wt_ref, wk, 3).wait()

    def k_step(t, carry):
        project_k(t)

        @pl.when(t == 0)
        def _():
            send_own(2)

        @pl.when(t > 0)
        def _():
            to_partner(0, t - 1).start()

        return carry

    lax.fori_loop(0, 3, k_step, 0)
    acc[...] = jnp.zeros_like(acc)
    sums[...] = jnp.zeros_like(sums)
    to_partner(0, 2).start()

    def weigh(s_ref, h_ref, j, diag_off):
        dots = s_ref[...]
        margin = dots * scale + bias
        if diag_off is not None:
            row_ids = lax.broadcasted_iota(jnp.int32, dots.shape, 0) + diag_off
            hit = row_ids == lax.broadcasted_iota(jnp.int32, dots.shape, 1)
            margin = jnp.where(hit, -margin, margin)
        exps = jnp.exp(-jnp.abs(margin))
        recip = 1.0 / (1.0 + exps)
        grad = jnp.where(margin >= 0, recip, exps * recip)
        if diag_off is not None:
            grad = jnp.where(hit, -grad, grad)
        h_ref[:, j * tile : (j + 1) * tile] = (grad * h_scale).astype(BF16)
        sums[0] += fold_log1p(exps) + fold_sum(jnp.maximum(margin, 0.0))
        sums[1] += fold_sum(grad * dots)
        sums[2] += fold_sum(grad)

    def attend(q0, tiles, slot, k0, blocks, diag):
        depth = blocks * tile
        cells = [(t, j) for t in range(tiles) for j in range(blocks)]
        pending = []
        half = dim // 2

        def q_at(t):
            return pl.ds(pl.multiple_of(q0 + t * qt, qt), qt)

        def gradient(t, n):
            at = q_at(t)
            cols = slice(n * half, (n + 1) * half)
            keys = kbuf[slot, pl.ds(pl.multiple_of(k0, tile), depth), cols]
            acc[at, cols] += jnp.dot(hblk[t % 2][:, :depth], keys, preferred_element_type=F32)

        for n in range(len(cells) + 1):
            if n < len(cells):
                t, j = cells[n]
                keys = kbuf[slot, pl.ds(pl.multiple_of(k0 + j * tile, tile), tile), :]
                sblk[n % 2][...] = lax.dot_general(eq[q_at(t), :], keys, (((1,), (1,)), ((), ())), preferred_element_type=F32)
            for _ in range(2 if blocks == 1 else 1):
                if pending:
                    gradient(*pending.pop(0))
            if n:
                t, j = cells[n - 1]
                weigh(sblk[(n - 1) % 2], hblk[t % 2], j, t * qt - j * tile if diag else None)
                if j == blocks - 1:
                    pending += [(t, 0), (t, 1)]
        for item in pending:
            gradient(*item)

    def take(slot, forward):
        for t in range(3):
            got(slot, t)
            if forward:
                to_partner(slot, t).start()

    attend(0, 2, 0, 0, 3, True)

    def first_step(i, carry):
        slot = i + 1

        @pl.when(slot == 2)
        def _():
            take(2, True)

        @pl.when(slot != 2)
        def _():
            for t in range(3):
                got(slot, t)

        attend(0, 2, slot, 0, 3, False)
        return carry

    lax.fori_loop(0, 2, first_step, 0)

    swap_copy.wait()

    def swp_step(t, carry):
        project_q(rows, t)

        @pl.when(t > 0)
        def _():
            swp_to_dst(t - 1).start()

        return carry

    lax.fori_loop(0, 3, swp_step, 0)

    def second_step(i, carry):
        @pl.when(i == 0)
        def _():
            swp_to_dst(2).start()

        @pl.when(i == 2)
        def _():
            take(3, False)

        slot = jnp.where(i < 2, i, jnp.where(i == 2, 3, i - 1))
        attend(jnp.where(i == 2, 0, rows), 2, slot, 0, 3, False)
        return carry

    lax.fori_loop(0, 5, second_step, 0)

    take(4, True)
    attend(rows, 2, 4, 0, 3, True)

    def third_step(i, carry):
        @pl.when(i == 1)
        def _():
            take(5, False)

        attend(jnp.where(i == 2, rows, 0), 2, jnp.where(i == 0, 4, 5), 0, 3, False)
        return carry

    lax.fori_loop(0, 3, third_step, 0)

    def last_step(i, carry):
        t, side = i // 2, i % 2

        @pl.when(side == 0)
        def _():
            got(6, t)
            to_partner(6, t).start()

        @pl.when(side == 1)
        def _():
            got(7, t)

        attend(0, 4, 6 + side, t * tile, 1, False)
        return carry

    lax.fori_loop(0, 6, last_step, 0)

    def back_step(t, carry):
        at = pl.ds(pl.multiple_of(t * tile, tile), tile)
        grad, val = acc[at], unit[at]
        proj = jnp.sum(val * grad, axis=1, keepdims=True)
        eq[at] = (inv[at][:, :1] * (grad - val * proj)).astype(BF16)
        return carry

    for t in range(3):
        own_to_dst(t).wait_send()
        own_to_src(t).wait_send()
        swp_to_dst(t).wait_send()
        for slot in (0, 2, 4, 6):
            to_partner(slot, t).wait_send()
    lax.fori_loop(0, 6, back_step, 0)

    def dw_step(t, carry):
        cols = pl.ds(pl.multiple_of(t * 256, 256), 256)
        dw_ref[cols, :] = lax.dot_general(xq[:, cols], eq[...], (((0,), (0,)), ((), ())), preferred_element_type=F32)
        return carry

    lax.fori_loop(0, dim // 256, dw_step, 0)
    lane = jnp.sum(sums[...], axis=1)
    scal_ref[...] = jnp.concatenate([lane[:, :128] + lane[:, 128:], jnp.zeros((5, 128), F32)], axis=0)


def reduce_kernel(n, dw_ref, scal_ref, img_out, txt_out, scal_out,
                  half, ysum, zsum, bufh, bufa, bufb, bufa2, bufb2, part, bufx, mine, other, sc_c, sc_y, sc_z, sc_x,
                  h_sem, a_sem, b_sem, a2_sem, b2_sem, x_sem, c_sem, ga_sem, ha_sem, gb_sem, hb_sem,
                  f_sem, m_sem, o_sem, out_sem):
    cut = (n * 5 // 8) // 128 * 128
    hr = n // 2
    ra, rb = hr // Y_N, hr // Z_N
    rf = hr // (Y_N * Z_N)
    rep = lax.axis_index("rep")
    dat = lax.axis_index("data")
    x, c = dat // 2, dat % 2
    z, y = rep // Y_N, rep % Y_N
    kind = x % 2
    step = 1 - 2 * c
    partner = (rep, x * 2 + 1 - c)
    dst = (rep, (x + step + X_N) % X_N * 2 + c)

    def at_y(d):
        return (z * Y_N + (y + d) % Y_N, dat)

    def at_z(d):
        return ((z + d) % Z_N * Y_N + y, dat)

    def at_x(d):
        return (rep, (x + d) % X_N * 2 + c)

    greet([partner] + [at_y(d) for d in range(1, Y_N)] + [at_z(d) for d in range(1, Z_N)] + [at_x(d) for d in range(1, X_N)])
    col_a, col_b = pl.ds(0, cut), pl.ds(cut, n - cut)

    def rows(start, size):
        return pl.ds(pl.multiple_of(start, 8), size)

    def pair(sem, i, src, dst_ref, peer):
        return remote(src, dst_ref, sem.at[0, i], sem.at[1, i], peer)

    def put(ref, i, peer_list, sem):
        copies = [pair(sem, k, ref.at[i], ref.at[i], peer) for k, peer in enumerate(peer_list)]
        for copy in copies:
            copy.start()
        return copies

    sends = []

    def launch(copy):
        copy.start()
        sends.append(copy)

    sc_c[c] = scal_ref[...]
    h_copy = pair(h_sem, 0, dw_ref.at[rows((1 - c) * hr, hr)], bufh, partner)
    launch(h_copy)
    cc = pair(c_sem, 0, sc_c.at[c], sc_c.at[c], partner)
    launch(cc)
    h_copy.wait_recv()
    half[...] = dw_ref[rows(c * hr, hr), :] + bufh[...]

    a_copies = [pair(a_sem, d - 1, half.at[rows((y + d) % Y_N * ra, ra), col_a], bufa.at[d - 1], at_y(d)) for d in range(1, Y_N)]
    b_copies = [pair(b_sem, d - 1, half.at[rows((z + d) % Z_N * rb, rb), col_b], bufb.at[d - 1], at_z(d)) for d in range(1, Z_N)]
    for copy in a_copies + b_copies:
        launch(copy)
    cc.wait_recv()
    sc_y[y] = sc_c[0] + sc_c[1]
    y_copies = [pair(c_sem, d, sc_y.at[y], sc_y.at[y], at_y(d)) for d in range(1, Y_N)]
    for copy in y_copies:
        launch(copy)

    for copy in a_copies:
        copy.wait_recv()
    tot = half[rows(y * ra, ra), 0:cut]
    for d in range(1, Y_N):
        tot = tot + bufa[d - 1]
    ysum[...] = tot
    a2_copies = [pair(a2_sem, d - 1, ysum.at[rows((z + d) % Z_N * rf, rf)], bufa2.at[d - 1], at_z(d)) for d in range(1, Z_N)]
    for copy in a2_copies:
        launch(copy)
    for copy in b_copies:
        copy.wait_recv()
    tot = half[rows(z * rb, rb), cut:n]
    for d in range(1, Z_N):
        tot = tot + bufb[d - 1]
    zsum[...] = tot
    b2_copies = [pair(b2_sem, d - 1, zsum.at[rows((y + d) % Y_N * rf, rf)], bufb2.at[d - 1], at_y(d)) for d in range(1, Y_N)]
    for copy in b2_copies:
        launch(copy)

    for copy in y_copies:
        copy.wait_recv()
    tot = sc_y[0]
    for i in range(1, Y_N):
        tot = tot + sc_y[i]
    sc_z[z] = tot
    z_copies = [pair(c_sem, Y_N + d, sc_z.at[z], sc_z.at[z], at_z(d)) for d in range(1, Z_N)]
    for copy in z_copies:
        launch(copy)

    for copy in a2_copies:
        copy.wait_recv()
    tot = ysum[rows(z * rf, rf), :]
    for d in range(1, Z_N):
        tot = tot + bufa2[d - 1]
    part[:, 0:cut] = tot
    for copy in b2_copies:
        copy.wait_recv()
    tot = zsum[rows(y * rf, rf), :]
    for d in range(1, Y_N):
        tot = tot + bufb2[d - 1]
    part[:, cut:n] = tot
    x_copy = pair(x_sem, 0, part, bufx, at_x(2))
    launch(x_copy)

    for copy in z_copies:
        copy.wait_recv()
    tot = sc_z[0]
    for i in range(1, Z_N):
        tot = tot + sc_z[i]
    sc_x[x] = tot
    s_copies = [pair(c_sem, Y_N + Z_N + d, sc_x.at[x], sc_x.at[x], at_x(d)) for d in range(1, X_N)]
    for copy in s_copies:
        launch(copy)

    x_copy.wait_recv()
    base = c * hr
    fin_a = rows(base + y * ra + z * rf, rf)
    fin_b = rows(base + z * rb + y * rf, rf)
    mine[fin_a, 0:cut] = part[:, 0:cut] + bufx[:, 0:cut]
    mine[fin_b, cut:n] = part[:, cut:n] + bufx[:, cut:n]

    def same(sem, i, ref, at, peer):
        return pair(sem, i, ref.at[at], ref.at[at], peer)

    ga = [same(ga_sem, d - 1, mine, (fin_a, col_a), at_z(d)) for d in range(1, Z_N)]
    gb = [same(gb_sem, d - 1, mine, (fin_b, col_b), at_y(d)) for d in range(1, Y_N)]
    for copy in gb + ga:
        launch(copy)
    for copy in s_copies:
        copy.wait_recv()
    tot = sc_x[0]
    for i in range(1, X_N):
        tot = tot + sc_x[i]
    scal_out[...] = tot

    def piece(i):
        if i < Y_N:
            return (rows(base + (y - i + Y_N) % Y_N * ra, ra), col_a)
        i -= Y_N
        return (rows(base + (z - i + Z_N) % Z_N * rb, rb), col_b)

    def partner_piece(i):
        pbase = (1 - c) * hr
        if i < Y_N:
            return (rows(pbase + (y - i + Y_N) % Y_N * ra, ra), col_a)
        i -= Y_N
        return (rows(pbase + (z - i + Z_N) % Z_N * rb, rb), col_b)

    def spread(i):
        launch(pair(f_sem, i, mine.at[piece(i)], other.at[piece(i)], dst))
        launch(same(m_sem, i, mine, piece(i), partner))

    for copy in gb:
        copy.wait_recv()
    hb = [same(hb_sem, d - 1, mine, piece(Y_N), at_z(d)) for d in range(1, Z_N)]
    for copy in hb:
        launch(copy)
    spread(Y_N)
    for copy in ga:
        copy.wait_recv()
    ha = [same(ha_sem, d - 1, mine, piece(0), at_y(d)) for d in range(1, Y_N)]
    for copy in ha:
        launch(copy)
    spread(0)

    def wait_piece(copy_sem, i, at):
        pair(copy_sem, i, mine.at[at], mine.at[at], partner).wait_recv()

    ring = [(min(d, Z_N - d) / Z_N, hb_sem, d) for d in range(1, Z_N)] + [(min(d, Y_N - d) / Y_N, ha_sem, d) for d in range(1, Y_N)]
    order = [(sem, d) for _, sem, d in sorted(ring, key=lambda item: item[0])]
    arrived = [Y_N, 0]
    for sem, d in order:
        i = d if sem is ha_sem else Y_N + d
        wait_piece(sem, d - 1, piece(i))
        spread(i)
        arrived.append(i)
    for i in arrived:
        pair(f_sem, i, other.at[piece(i)], other.at[piece(i)], dst).wait_recv()
        launch(same(o_sem, i, other, piece(i), partner))
    for i in arrived:
        wait_piece(m_sem, i, partner_piece(i))
    for i in arrived:
        wait_piece(o_sem, i, partner_piece(i))
    for copy in sends:
        copy.wait_send()

    def store(i, from_ref, to_ref):
        return pltpu.make_async_copy(from_ref, to_ref, out_sem.at[i])

    @pl.when(kind == 0)
    def _():
        store(0, mine, img_out).start()
        store(1, other, txt_out).start()

    @pl.when(kind == 1)
    def _():
        store(0, mine, txt_out).start()
        store(1, other, img_out).start()

    store(0, mine, img_out).wait()
    store(1, other, txt_out).wait()


def pair_sems(count):
    return pltpu.SemaphoreType.DMA((2, count))


def head_gradients(img_loc, txt_loc, w_img, w_txt, log_temp, logit_bias, total_rows):
    rows, dim = img_loc.shape
    temp_scale = jnp.exp(log_temp)
    sc = jnp.stack([temp_scale, logit_bias])
    any_spec = pl.BlockSpec(memory_space=pl.ANY)
    vmem_spec = pl.BlockSpec(memory_space=pltpu.VMEM)
    tile, qt = rows // 3, rows // 2
    dma = pltpu.SemaphoreType.DMA
    flops = 2 * rows * dim * dim * 7 + 4 * 2 * rows * 8 * rows * dim
    dw, scal = pl.pallas_call(
        functools.partial(main_kernel, total_rows, rows, dim),
        out_shape=(jax.ShapeDtypeStruct((dim, dim), F32), jax.ShapeDtypeStruct((8, 128), F32)),
        in_specs=[pl.BlockSpec(memory_space=pltpu.SMEM)] + [any_spec] * 4,
        out_specs=(vmem_spec, vmem_spec),
        scratch_shapes=[
            pltpu.VMEM((2 * rows, dim), BF16),
            pltpu.VMEM((rows, dim), BF16),
            pltpu.VMEM((dim, dim), BF16),
            pltpu.VMEM((dim, dim), BF16),
            pltpu.VMEM((8, rows, dim), BF16),
            pltpu.VMEM((2 * rows, dim), BF16),
            pltpu.VMEM((2 * rows, dim), F32),
            pltpu.VMEM((2 * rows, 128), F32),
            pltpu.VMEM((2 * rows, dim), F32),
            pltpu.VMEM((qt, tile), F32),
            pltpu.VMEM((qt, tile), F32),
            pltpu.VMEM((qt, rows), BF16),
            pltpu.VMEM((qt, rows), BF16),
            pltpu.VMEM((3, 8, tile), F32),
            dma((4,)), dma, dma, dma((7, 3)), dma((8, 3)),
        ],
        compiler_params=pltpu.CompilerParams(collective_id=0, has_side_effects=True, vmem_limit_bytes=VMEM_CAP),
        cost_estimate=pl.CostEstimate(flops=flops, bytes_accessed=16 << 20, transcendentals=0),
        name="contrast",
    )(sc, img_loc, txt_loc, w_img, w_txt)

    cut = (dim * 5 // 8) // 128 * 128
    hr = dim // 2
    ra, rb, rf = hr // Y_N, hr // Z_N, hr // (Y_N * Z_N)
    nb = dim - cut
    dw_img, dw_txt, scal = pl.pallas_call(
        functools.partial(reduce_kernel, dim),
        out_shape=(jax.ShapeDtypeStruct((dim, dim), F32), jax.ShapeDtypeStruct((dim, dim), F32), jax.ShapeDtypeStruct((8, 128), F32)),
        in_specs=[vmem_spec, vmem_spec],
        out_specs=(any_spec, any_spec, vmem_spec),
        scratch_shapes=[
            pltpu.VMEM((hr, dim), F32),
            pltpu.VMEM((ra, cut), F32),
            pltpu.VMEM((rb, nb), F32),
            pltpu.VMEM((hr, dim), F32),
            pltpu.VMEM((Y_N - 1, ra, cut), F32),
            pltpu.VMEM((Z_N - 1, rb, nb), F32),
            pltpu.VMEM((Z_N - 1, rf, cut), F32),
            pltpu.VMEM((Y_N - 1, rf, nb), F32),
            pltpu.VMEM((rf, dim), F32),
            pltpu.VMEM((rf, dim), F32),
            pltpu.VMEM((dim, dim), F32),
            pltpu.VMEM((dim, dim), F32),
            pltpu.VMEM((C_N, 8, 128), F32),
            pltpu.VMEM((Y_N, 8, 128), F32),
            pltpu.VMEM((Z_N, 8, 128), F32),
            pltpu.VMEM((X_N, 8, 128), F32),
            pair_sems(1), pair_sems(Y_N - 1), pair_sems(Z_N - 1), pair_sems(Z_N - 1), pair_sems(Y_N - 1),
            pair_sems(1), pair_sems(X_N + Y_N + Z_N), pair_sems(Z_N - 1), pair_sems(Y_N - 1), pair_sems(Y_N - 1),
            pair_sems(Z_N - 1), pair_sems(Y_N + Z_N), pair_sems(Y_N + Z_N), pair_sems(Y_N + Z_N), dma((2,)),
        ],
        compiler_params=pltpu.CompilerParams(collective_id=1, has_side_effects=True, vmem_limit_bytes=VMEM_CAP),
        name="head_sum",
    )(dw, scal)
    tot = jnp.sum(scal, axis=1) * 0.5
    inv_n = F32(1.0 / total_rows)
    return tot[0] * inv_n, temp_scale * tot[1] * inv_n, tot[2] * inv_n, dw_img, dw_txt


def solution(mesh):
    devices = mesh.shape["rep"] * mesh.shape["data"]
    row_spec = P(("rep", "data"), None)

    def device_body(img_loc, txt_loc, w_img, w_txt, log_temp, logit_bias):
        return head_gradients(img_loc, txt_loc, w_img, w_txt, log_temp, logit_bias, img_loc.shape[0] * devices)

    return jax.shard_map(device_body, mesh=mesh, in_specs=(row_spec, row_spec, P(), P(), P(), P()), out_specs=(P(), P(), P(), P(), P()), check_vma=False)
```

```python
import functools

import jax
import jax.numpy as jnp
from jax import lax
from jax.experimental import pallas as pl
from jax.experimental.pallas import tpu as pltpu
from jax.sharding import PartitionSpec as P

F32 = jnp.float32
BF16 = jnp.bfloat16
MESH = pl.DeviceIdType.MESH
X_N, C_N, Y_N, Z_N = 4, 2, 4, 8
VMEM_CAP = 55 << 20


def greet(peers):
    barrier = pltpu.get_barrier_semaphore()
    for peer in peers:
        pl.semaphore_signal(barrier, inc=1, device_id=peer, device_id_type=MESH)
    pl.semaphore_wait(barrier, len(peers))


def remote(src, dst, send_sem, recv_sem, peer):
    return pltpu.make_async_remote_copy(
        src_ref=src, dst_ref=dst, send_sem=send_sem, recv_sem=recv_sem, device_id=peer, device_id_type=MESH
    )


def fold_sum(val):
    rows, cols = val.shape
    return jnp.sum(val.reshape(rows // 8, 8, cols), axis=0)


def whole_kernel(total_rows, rows, dim, cut, sc_ref, img_ref, txt_ref, wi_ref, wt_ref, img_out, txt_out, scal_out,
                xq, xk, wq, wk, kbuf, eq, unit, inv, acc, sblk0, sblk1, hblk0, hblk1, sums, away, landed,
                half,
                ysum, zsum, ylow, yhigh, yring, bufb, bufa2, bufb2, part, bufx, sc_c, sc_y, sc_z, sc_x,
                ld_sem, xs_sem, xr_sem, es_sem, er_sem, ps_sem, pr_sem, hs_sem, hr_sem,
                l_sem, k_sem, b_sem, a2_sem, b2_sem, x_sem, c_sem, ga_sem, ha_sem, gb_sem, hb_sem,
                f_sem, m_sem, o_sem, fin_sem):
    n = dim
    tile = rows // 3
    qt = rows // 2
    rep = lax.axis_index("rep")
    dat = lax.axis_index("data")
    x, c = dat // 2, dat % 2
    kind = x % 2
    step = 1 - 2 * c
    dst_x = (x + step + X_N) % X_N
    src_x = (x - step + X_N) % X_N
    partner = (rep, x * 2 + 1 - c)
    dst = (rep, dst_x * 2 + c)
    src = (rep, src_x * 2 + c)
    scale, bias = sc_ref[0], sc_ref[1]
    h_scale = scale * F32(1.0 / total_rows)
    log2_e = F32(1.4426950408889634)
    scale2, bias2 = scale * log2_e, bias * log2_e
    sblk = (sblk0, sblk1)
    hblk = (hblk0, hblk1)

    z, y = rep // Y_N, rep % Y_N

    def at_y(d):
        return (z * Y_N + (y + d + Y_N) % Y_N, dat)

    def at_z(d):
        return ((z + d) % Z_N * Y_N + y, dat)

    def at_x(d):
        return (rep, (x + d) % X_N * 2 + c)

    up, down = at_y(1), at_y(-1)

    def load(from_ref, to_ref, idx):
        return pltpu.make_async_copy(from_ref, to_ref, ld_sem.at[idx])

    own = pl.ds(0, rows)
    swp = pl.ds(rows, rows)

    @pl.when(kind == 0)
    def _():
        load(txt_ref, xk, 0).start()
        load(img_ref, xq.at[own], 1).start()
        load(wi_ref, wq, 2).start()
        load(wt_ref, wk, 3).start()

    @pl.when(kind == 1)
    def _():
        load(img_ref, xk, 0).start()
        load(txt_ref, xq.at[own], 1).start()
        load(wt_ref, wq, 2).start()
        load(wi_ref, wk, 3).start()

    greet([partner] + [at_y(d) for d in range(1, Y_N)] + [at_z(d) for d in range(1, Z_N)] + [at_x(d) for d in range(1, X_N)])
    load(txt_ref, xk, 0).wait()
    swap_copy = remote(xk, xq.at[swp], xs_sem, xr_sem, dst)
    swap_copy.start()

    def direct(g):
        return kbuf.at[g, pl.ds(0, tile)]

    def passed(g):
        return kbuf.at[g, pl.ds(tile, tile)]

    def erows(base, t):
        return eq.at[pl.ds(pl.multiple_of(base + t * tile, tile), tile)]

    def own_to_src(t):
        return remote(erows(0, t), direct(3 + t), es_sem.at[t], er_sem.at[t], src)

    def own_to_dst(t):
        return remote(erows(0, t), direct(6 + t), es_sem.at[3 + t], er_sem.at[3 + t], dst)

    def swp_to_dst(t):
        return remote(erows(rows, t), direct(9 + t), es_sem.at[6 + t], er_sem.at[6 + t], dst)

    def got_direct(g):
        remote(direct(g), direct(g), es_sem.at[0], er_sem.at[g - 3], partner).wait_recv()

    def pass_own(t):
        return remote(direct(t), passed(t), ps_sem.at[t], pr_sem.at[t], partner)

    def pass_on(g):
        return remote(direct(g), passed(g + 1), ps_sem.at[g], pr_sem.at[g], partner)

    def got_passed(i):
        remote(passed(0), passed(0), ps_sem.at[i], pr_sem.at[i], partner).wait_recv()

    def project_q(base, t):
        at = pl.ds(pl.multiple_of(base + t * tile, tile), tile)
        raw = jnp.dot(xq[at], wq[...], preferred_element_type=F32)
        inv_norm = lax.rsqrt(jnp.sum(raw * raw, axis=1, keepdims=True))
        val = raw * inv_norm
        unit[at] = val
        eq[at] = val.astype(BF16)
        inv[at] = jnp.broadcast_to(inv_norm, (tile, 128))

    def project_k(t):
        at = pl.ds(pl.multiple_of(t * tile, tile), tile)
        raw = jnp.dot(xk[at], wk[...], preferred_element_type=F32)
        inv_norm = lax.rsqrt(jnp.sum(raw * raw, axis=1, keepdims=True))
        kbuf[t, :tile] = (raw * inv_norm).astype(BF16)

    load(wt_ref, wk, 3).wait()

    def k_step(t, carry):
        project_k(t)

        @pl.when(t > 0)
        def _():
            pass_own(t - 1).start()

        return carry

    lax.fori_loop(0, 3, k_step, 0)
    load(img_ref, xq.at[own], 1).wait()
    load(wi_ref, wq, 2).wait()

    def own_step(t, carry):
        project_q(0, t)

        @pl.when(t == 0)
        def _():
            pass_own(2).start()

        return carry

    lax.fori_loop(0, 3, own_step, 0)
    acc[...] = jnp.zeros_like(acc)
    sums[...] = jnp.zeros_like(sums)

    def weigh(s_ref, h_ref, j, diag_off):
        loss, temp, tilt, lift = None, None, None, None
        for r in range(0, qt, 32):
            dots = s_ref[r : r + 32, slice(j * tile, (j + 1) * tile)]
            logit = dots * scale2 + bias2
            if diag_off is not None:
                row_ids = lax.broadcasted_iota(jnp.int32, dots.shape, 0) + (diag_off + r)
                hit = row_ids == lax.broadcasted_iota(jnp.int32, dots.shape, 1)
                logit = jnp.where(hit, -logit, logit)
            exps = jnp.exp2(jnp.minimum(logit, -logit))
            grad = jnp.exp2(jnp.minimum(logit, 0.0)) * (1.0 / (1.0 + exps))
            if diag_off is not None:
                grad = jnp.where(hit, -grad, grad)
            h_ref[r : r + 32, j * tile : (j + 1) * tile] = (grad * h_scale).astype(BF16)
            parts = [exps[i : i + 8] for i in range(0, 32, 8)]
            while len(parts) > 1:
                parts = [a + b + a * b for a, b in zip(parts[::2], parts[1::2])]
            one, two, three = fold_sum(grad * dots), fold_sum(grad), fold_sum(jnp.maximum(logit, 0.0))
            if r:
                loss = loss + parts[0] + loss * parts[0]
                temp, tilt, lift = temp + one, tilt + two, lift + three
            else:
                loss, temp, tilt, lift = parts[0], one, two, three
        sums[0] += jnp.log1p(loss)
        sums[1] += temp
        sums[2] += tilt
        sums[3] += lift

    def attend(q0, tiles, g, k0, blocks, diag_from, key_tile):
        depth = blocks * tile
        pending = []
        mid = dim // 2

        def gradient(t, n):
            at = slice(q0 + t * qt, q0 + (t + 1) * qt)
            cols = slice(n * mid, (n + 1) * mid)
            acc[at, cols] += jnp.dot(hblk[t % 2][:, :depth], kbuf[g, k0 : k0 + depth, cols], preferred_element_type=F32)

        for t in range(tiles + 1):
            if t < tiles:
                ques = eq[q0 + t * qt : q0 + (t + 1) * qt, :]
                sblk[t % 2][:, :depth] = lax.dot_general(ques, kbuf[g, k0 : k0 + depth, :], (((1,), (1,)), ((), ())), preferred_element_type=F32)
            for item in pending:
                gradient(*item)
            pending = []
            if t:
                for j in range(blocks):
                    diag = diag_from is not None and t - 1 >= diag_from and j == 0
                    weigh(sblk[(t - 1) % 2], hblk[(t - 1) % 2], j, (t - 1 - diag_from) * qt - key_tile * tile if diag else None)
                pending = [(t - 1, 0), (t - 1, 1)]
        for item in pending:
            gradient(*item)

    def first_step(t, carry):
        got_passed(t)
        attend(0, 2, t, 0, 2, 0, t)
        return carry

    lax.fori_loop(0, 3, first_step, 0)

    swap_copy.wait_send()
    for t in range(3):
        own_to_src(t).start()
    swap_copy.wait_recv()

    def swp_step(t, carry):
        project_q(rows, t)
        return carry

    lax.fori_loop(0, 3, swp_step, 0)

    def second_step(t, carry):
        @pl.when(t == 2)
        def _():
            for i in range(3):
                own_to_dst(i).start()
            for i in range(3):
                swp_to_dst(i).start()
            got_direct(3)
            pass_on(3).start()

        attend(rows, 2, t, 0, 2, None, None)
        return carry

    lax.fori_loop(0, 3, second_step, 0)
    attend(0, 4, 3, 0, 1, None, None)

    def main_step(g, carry):
        got_direct(g)
        pass_on(g).start()
        got_passed(g - 1)
        twin = (g >= 6) & (g < 9)

        @pl.when(twin)
        def _():
            attend(0, 4, g, 0, 2, 2, g - 6)

        @pl.when(jnp.logical_not(twin))
        def _():
            attend(0, 4, g, 0, 2, None, None)

        return carry

    lax.fori_loop(4, 12, main_step, 0)
    got_passed(11)
    attend(0, 4, 12, tile, 1, None, None)

    for t in range(3):
        own_to_src(t).wait_send()
        own_to_dst(t).wait_send()
        swp_to_dst(t).wait_send()

    def back_step(t, carry):
        at = pl.ds(pl.multiple_of(t * tile, tile), tile)
        grad, val = acc[at], unit[at]
        proj = jnp.sum(val * grad, axis=1, keepdims=True)
        eq[at] = (inv[at][:, :1] * (grad - val * proj)).astype(BF16)
        return carry

    lax.fori_loop(0, 6, back_step, 0)

    strip = dim // 8
    hrows = dim // 2

    def head(row0, n):
        cols = pl.ds(pl.multiple_of(row0, strip), n)
        return lax.dot_general(xq[:, cols], eq[...], (((0,), (0,)), ((), ())), preferred_element_type=F32)

    def give(t):
        at = pl.ds(pl.multiple_of(t * 2 * strip, strip), 2 * strip)
        return remote(away.at[at], landed.at[at], hs_sem.at[t], hr_sem.at[t], partner)

    def away_step(t, carry):
        away[pl.ds(pl.multiple_of(t * 2 * strip, strip), 2 * strip), :] = head((1 - c) * hrows + t * 2 * strip, 2 * strip)

        @pl.when(t == 1)
        def _():
            give(0).start()

        return carry

    lax.fori_loop(0, 2, away_step, 0)
    give(1).start()

    def home_step(t, carry):
        at = pl.ds(pl.multiple_of(t * 2 * strip, strip), 2 * strip)
        half[at, :] = head(c * hrows + t * 2 * strip, 2 * strip)
        return carry

    lax.fori_loop(0, 2, home_step, 0)
    give(0).wait_recv()
    give(1).wait_recv()

    def join_step(t, carry):
        at = pl.ds(pl.multiple_of(t * strip, strip), strip)
        half[at, :] += landed[at, :]
        return carry

    lax.fori_loop(0, 4, join_step, 0)
    lane = jnp.sum(sums[...], axis=1)
    lane = lane[:, :128] + lane[:, 128:]
    loss = lane[:1] + lane[3:] * F32(0.6931471805599453)
    sc_c[c] = jnp.concatenate([loss, lane[1:3], jnp.zeros((5, 128), F32)], axis=0)
    for t in range(2):
        give(t).wait_send()
    for t in range(3):
        pass_own(t).wait_send()
    for g in range(3, 12):
        pass_on(g).wait_send()

    hr = n // 2
    ra, rb = hr // Y_N, hr // Z_N
    rf = hr // (Y_N * Z_N)
    hh = ra // 2
    col_a, col_b = pl.ds(0, cut), pl.ds(cut, n - cut)

    def rows(start, size):
        return pl.ds(pl.multiple_of(start, 8), size)

    def pair(sem, i, src, dst_ref, peer):
        return remote(src, dst_ref, sem.at[0, i], sem.at[1, i], peer)

    sends = []

    def launch(copy):
        copy.start()
        sends.append(copy)

    def block_y(d, part_rows=None):
        first, size = part_rows or (0, ra)
        return rows((y + d + Y_N) % Y_N * ra + first, size)

    low, high = (0, hh), (hh, hh)

    low_in = pair(l_sem, 0, half.at[block_y(2, low), col_a], ylow, up)
    high_in = pair(l_sem, 1, half.at[block_y(2, high), col_a], yhigh, down)
    own_up = pair(k_sem, 0, half.at[block_y(1, high), col_a], yring.at[0, pl.ds(hh, hh)], up)
    own_down = pair(k_sem, 1, half.at[block_y(-1, low), col_a], yring.at[1, pl.ds(0, hh)], down)
    sum_up = pair(k_sem, 2, ylow, yring.at[0, pl.ds(0, hh)], up)
    sum_down = pair(k_sem, 3, yhigh, yring.at[1, pl.ds(hh, hh)], down)
    b_copies = [pair(b_sem, d - 1, half.at[rows((z + d) % Z_N * rb, rb), col_b], bufb.at[d - 1], at_z(d)) for d in range(1, Z_N)]
    for copy in [low_in, high_in, own_up, own_down] + b_copies:
        launch(copy)
    cc = pair(c_sem, 0, sc_c.at[c], sc_c.at[c], partner)
    launch(cc)
    low_in.wait_recv()
    ylow[...] += half[block_y(1, low), 0:cut]
    high_in.wait_recv()
    yhigh[...] += half[block_y(-1, high), 0:cut]
    launch(sum_up)
    launch(sum_down)
    cc.wait_recv()
    sc_y[y] = sc_c[0] + sc_c[1]
    y_copies = [pair(c_sem, d, sc_y.at[y], sc_y.at[y], at_y(d)) for d in range(1, Y_N)]
    for copy in y_copies:
        launch(copy)

    for copy in [own_up, own_down, sum_up, sum_down]:
        copy.wait_recv()
    ysum[...] = (half[block_y(0), 0:cut] + yring[0]) + yring[1]
    a2_copies = [pair(a2_sem, d - 1, ysum.at[rows((z + d) % Z_N * rf, rf)], bufa2.at[d - 1], at_z(d)) for d in range(1, Z_N)]
    for copy in a2_copies:
        launch(copy)
    for copy in b_copies:
        copy.wait_recv()
    tot = half[rows(z * rb, rb), cut:n]
    for d in range(1, Z_N):
        tot = tot + bufb[d - 1]
    zsum[...] = tot
    b2_copies = [pair(b2_sem, d - 1, zsum.at[rows((y + d) % Y_N * rf, rf)], bufb2.at[d - 1], at_y(d)) for d in range(1, Y_N)]
    for copy in b2_copies:
        launch(copy)

    for copy in y_copies:
        copy.wait_recv()
    tot = sc_y[0]
    for i in range(1, Y_N):
        tot = tot + sc_y[i]
    sc_z[z] = tot
    z_copies = [pair(c_sem, Y_N + d, sc_z.at[z], sc_z.at[z], at_z(d)) for d in range(1, Z_N)]
    for copy in z_copies:
        launch(copy)

    for copy in a2_copies:
        copy.wait_recv()
    tot = ysum[rows(z * rf, rf), :]
    for d in range(1, Z_N):
        tot = tot + bufa2[d - 1]
    part[:, 0:cut] = tot
    for copy in b2_copies:
        copy.wait_recv()
    tot = zsum[rows(y * rf, rf), :]
    for d in range(1, Y_N):
        tot = tot + bufb2[d - 1]
    part[:, cut:n] = tot
    x_copy = pair(x_sem, 0, part, bufx.at[0], at_x(2))
    launch(x_copy)

    for copy in z_copies:
        copy.wait_recv()
    tot = sc_z[0]
    for i in range(1, Z_N):
        tot = tot + sc_z[i]
    sc_x[x] = tot
    s_copies = [pair(c_sem, Y_N + Z_N + d, sc_x.at[x], sc_x.at[x], at_x(d)) for d in range(1, X_N)]
    for copy in s_copies:
        launch(copy)

    x_copy.wait_recv()
    bufx[1] = part[...] + bufx[0]
    base = c * hr
    fin_a = rows(base + y * ra + z * rf, rf)
    fin_b = rows(base + z * rb + y * rf, rf)

    def by_kind(act):
        @pl.when(kind == 0)
        def _():
            act(img_out, txt_out)

        @pl.when(kind == 1)
        def _():
            act(txt_out, img_out)

    def same(sem, i, ref, at, peer):
        return pair(sem, i, ref.at[at], ref.at[at], peer)

    def put(mine, i, col, at):
        return pltpu.make_async_copy(bufx.at[1, :, col], mine.at[at, col], fin_sem.at[i])

    def gather_b(mine, d):
        return pair(gb_sem, d - 1, bufx.at[1, :, col_b], mine.at[fin_b, col_b], at_y(d))

    def gather_a(mine, d):
        return pair(ga_sem, d - 1, bufx.at[1, :, col_a], mine.at[fin_a, col_a], at_z(d))

    def first_gather(mine, other):
        for d in range(1, Y_N):
            gather_b(mine, d).start()
        for d in range(1, Z_N):
            gather_a(mine, d).start()
        put(mine, 0, col_a, fin_a).start()
        put(mine, 1, col_b, fin_b).start()

    by_kind(first_gather)
    for copy in s_copies:
        copy.wait_recv()
    tot = sc_x[0]
    for i in range(1, X_N):
        tot = tot + sc_x[i]
    scal_out[...] = tot
    put(img_out, 0, col_a, fin_a).wait()
    put(img_out, 1, col_b, fin_b).wait()

    def piece(i, core):
        if i < Y_N:
            return (rows(core * hr + (y - i + Y_N) % Y_N * ra, ra), col_a)
        return (rows(core * hr + (z - i + Y_N + Z_N) % Z_N * rb, rb), col_b)

    def quarter(d, part_rows):
        return (rows(base + (y + d + Y_N) % Y_N * ra + part_rows[0], part_rows[1]), col_a)

    def forward(mine, i):
        return pair(f_sem, i, mine.at[piece(i, c)], mine.at[piece(i, c)], dst)

    def spread(mine, other, i):
        forward(mine, i).start()
        same(m_sem, i, mine, piece(i, c), partner).start()

    def over_z(mine, d):
        return same(hb_sem, d - 1, mine, piece(Y_N, c), at_z(d))

    def full(mine, i):
        return same(ha_sem, i, mine, piece(0, c), up if i == 0 else down)

    def onward(mine, i):
        return same(ha_sem, 2 + i, mine, quarter(-1, low) if i == 0 else quarter(1, high), up if i == 0 else down)

    for d in range(1, Y_N):
        gather_b(img_out, d).wait_recv()

    def second_b(mine, other):
        for d in range(1, Z_N):
            over_z(mine, d).start()
        spread(mine, other, Y_N)

    by_kind(second_b)
    for d in range(1, Z_N):
        gather_a(img_out, d).wait_recv()

    def second_a(mine, other):
        full(mine, 0).start()
        full(mine, 1).start()
        spread(mine, other, 0)

    by_kind(second_a)

    def z_piece(d):
        same(hb_sem, d - 1, img_out, piece(Y_N + d, c), partner).wait_recv()

    z_piece(1)
    z_piece(Z_N - 1)
    for i in range(2):
        full(img_out, i).wait_recv()

    def third(mine, other):
        onward(mine, 0).start()
        onward(mine, 1).start()
        for i in (Y_N + 1, Y_N + Z_N - 1, 1, 3):
            spread(mine, other, i)

    by_kind(third)
    arrived = [Y_N, 0, Y_N + 1, Y_N + Z_N - 1, 1, 3]
    near = [d // 2 + 1 if d % 2 == 0 else Z_N - d // 2 - 1 for d in range(2, Z_N - 1)]
    for d in near[:2]:
        z_piece(d)
    by_kind(lambda mine, other: [spread(mine, other, Y_N + d) for d in near[:2]] and None)
    onward(img_out, 0).wait_recv()
    onward(img_out, 1).wait_recv()
    by_kind(lambda mine, other: spread(mine, other, 2))
    for d in near[2:]:
        z_piece(d)
    by_kind(lambda mine, other: [spread(mine, other, Y_N + d) for d in near[2:]] and None)
    arrived += [Y_N + d for d in near[:2]] + [2] + [Y_N + d for d in near[2:]]

    def across(group):
        for i in group:
            forward(img_out, i).wait_recv()
        by_kind(lambda mine, other: [same(o_sem, i, other, piece(i, c), partner).start() for i in group] and None)

    for at in range(0, len(arrived), 3):
        across(arrived[at : at + 3])
    for i in arrived:
        same(m_sem, i, img_out, piece(i, 1 - c), partner).wait_recv()
    for i in arrived:
        same(o_sem, i, img_out, piece(i, 1 - c), partner).wait_recv()
    for copy in sends:
        copy.wait_send()
    for d in range(1, Y_N):
        gather_b(img_out, d).wait_send()
    for d in range(1, Z_N):
        gather_a(img_out, d).wait_send()
        over_z(img_out, d).wait_send()
    for i in range(2):
        full(img_out, i).wait_send()
        onward(img_out, i).wait_send()
    for i in arrived:
        forward(img_out, i).wait_send()
        same(m_sem, i, img_out, piece(i, c), partner).wait_send()
        same(o_sem, i, img_out, piece(i, c), partner).wait_send()


def pair_sems(count):
    return pltpu.SemaphoreType.DMA((2, count))


def head_gradients(img_loc, txt_loc, w_img, w_txt, log_temp, logit_bias, total_rows):
    rows, dim = img_loc.shape
    temp_scale = jnp.exp(log_temp)
    sc = jnp.stack([temp_scale, logit_bias])
    any_spec = pl.BlockSpec(memory_space=pl.ANY)
    vmem_spec = pl.BlockSpec(memory_space=pltpu.VMEM)
    tile, qt = rows // 3, rows // 2
    dma = pltpu.SemaphoreType.DMA
    flops = 2 * rows * dim * dim * 7 + 4 * 2 * rows * 8 * rows * dim
    cut = (dim * 3 // 4) // 128 * 128
    hr = dim // 2
    ra, rb, rf = hr // Y_N, hr // Z_N, hr // (Y_N * Z_N)
    nb = dim - cut
    head = jax.ShapeDtypeStruct((dim, dim), F32)
    vmem = pltpu.VMEM
    dw_img, dw_txt, scal = pl.pallas_call(
        functools.partial(whole_kernel, total_rows, rows, dim, cut),
        out_shape=(head, head, jax.ShapeDtypeStruct((8, 128), F32)),
        in_specs=[pl.BlockSpec(memory_space=pltpu.SMEM)] + [any_spec] * 4,
        out_specs=(any_spec, any_spec, vmem_spec),
        scratch_shapes=[
            vmem((2 * rows, dim), BF16),
            vmem((rows, dim), BF16),
            vmem((dim, dim), BF16),
            vmem((dim, dim), BF16),
            vmem((13, 2 * tile, dim), BF16),
            vmem((2 * rows, dim), BF16),
            vmem((2 * rows, dim), F32),
            vmem((2 * rows, 128), F32),
            vmem((2 * rows, dim), F32),
            vmem((qt, 2 * tile), F32),
            vmem((qt, 2 * tile), F32),
            vmem((qt, 2 * tile), BF16),
            vmem((qt, 2 * tile), BF16),
            vmem((4, 8, tile), F32),
            vmem((hr, dim), F32),
            vmem((hr, dim), F32),
            vmem((hr, dim), F32),
            vmem((ra, cut), F32),
            vmem((rb, nb), F32),
            vmem((ra // 2, cut), F32),
            vmem((ra // 2, cut), F32),
            vmem((2, ra, cut), F32),
            vmem((Z_N - 1, rb, nb), F32),
            vmem((Z_N - 1, rf, cut), F32),
            vmem((Y_N - 1, rf, nb), F32),
            vmem((rf, dim), F32),
            vmem((2, rf, dim), F32),
            vmem((C_N, 8, 128), F32),
            vmem((Y_N, 8, 128), F32),
            vmem((Z_N, 8, 128), F32),
            vmem((X_N, 8, 128), F32),
            dma((4,)), dma, dma, dma((9,)), dma((9,)), dma((12,)), dma((12,)), dma((2,)), dma((2,)),
            pair_sems(2), pair_sems(4), pair_sems(Z_N - 1), pair_sems(Z_N - 1), pair_sems(Y_N - 1),
            pair_sems(1), pair_sems(X_N + Y_N + Z_N), pair_sems(Z_N - 1), pair_sems(4), pair_sems(Y_N - 1),
            pair_sems(Z_N - 1), pair_sems(Y_N + Z_N), pair_sems(Y_N + Z_N), pair_sems(Y_N + Z_N), dma((2,)),
        ],
        compiler_params=pltpu.CompilerParams(collective_id=0, has_side_effects=True, vmem_limit_bytes=VMEM_CAP),
        cost_estimate=pl.CostEstimate(flops=flops, bytes_accessed=16 << 20, transcendentals=0),
        name="contrast",
    )(sc, img_loc, txt_loc, w_img, w_txt)
    tot = jnp.sum(scal, axis=1) * 0.5
    inv_n = F32(1.0 / total_rows)
    return tot[0] * inv_n, temp_scale * tot[1] * inv_n, tot[2] * inv_n, dw_img, dw_txt


def solution(mesh):
    devices = mesh.shape["rep"] * mesh.shape["data"]
    row_spec = P(("rep", "data"), None)

    def device_body(img_loc, txt_loc, w_img, w_txt, log_temp, logit_bias):
        return head_gradients(img_loc, txt_loc, w_img, w_txt, log_temp, logit_bias, img_loc.shape[0] * devices)

    return jax.shard_map(device_body, mesh=mesh, in_specs=(row_spec, row_spec, P(), P(), P(), P()), out_specs=(P(), P(), P(), P(), P()), check_vma=False)
```

```python
import functools

import jax
import jax.numpy as jnp
from jax import lax
from jax.experimental import pallas as pl
from jax.experimental.pallas import tpu as pltpu
from jax.sharding import PartitionSpec as P

F32 = jnp.float32
BF16 = jnp.bfloat16
MESH = pl.DeviceIdType.MESH
X_N, C_N, Y_N, Z_N = 4, 2, 4, 8
VMEM_CAP = 67_043_328


def greet(peers):
    barrier = pltpu.get_barrier_semaphore()
    for peer in peers:
        pl.semaphore_signal(barrier, inc=1, device_id=peer, device_id_type=MESH)
    pl.semaphore_wait(barrier, len(peers))


def remote(src, dst, send_sem, recv_sem, peer):
    return pltpu.make_async_remote_copy(
        src_ref=src, dst_ref=dst, send_sem=send_sem, recv_sem=recv_sem, device_id=peer, device_id_type=MESH
    )


def fold_sum(val):
    rows, cols = val.shape
    return jnp.sum(val.reshape(rows // 8, 8, cols), axis=0)


def whole_kernel(total_rows, rows, dim, cut, lt_ref, lb_ref, img_ref, txt_ref, wi_ref, wt_ref,
                 img_out, txt_out, loss_out, temp_out, bias_out,
                xq, xk, wq, wk, kbuf, eq, unit, inv, acc, sblk0, sblk1, hblk0, hblk1, sums, away, landed,
                half,
                ysum, zsum, ylow, yhigh, yring, bufb, bufa2, bufb2, part, bufx, sc_c, sc_y, sc_z, sc_x,
                ld_sem, xs_sem, xr_sem, es_sem, er_sem, ps_sem, pr_sem, hs_sem, hr_sem,
                l_sem, k_sem, b_sem, a2_sem, b2_sem, x_sem, c_sem, ga_sem, ha_sem, gb_sem, hb_sem,
                f_sem, m_sem, o_sem, fin_sem):
    n = dim
    tile = rows // 3
    qt = rows // 2
    rep = lax.axis_index("rep")
    dat = lax.axis_index("data")
    x, c = dat // 2, dat % 2
    kind = x % 2
    step = 1 - 2 * c
    dst_x = (x + step + X_N) % X_N
    src_x = (x - step + X_N) % X_N
    partner = (rep, x * 2 + 1 - c)
    dst = (rep, dst_x * 2 + c)
    src = (rep, src_x * 2 + c)
    inv_n = F32(1.0 / total_rows)
    log2_e = F32(1.4426950408889634)
    temp = jnp.exp(jnp.full((1, tile), lt_ref[0], F32))
    h_scale, scale2, bias2 = temp * inv_n, temp * log2_e, lb_ref[0] * log2_e
    sblk = (sblk0, sblk1)
    hblk = (hblk0, hblk1)

    z, y = rep // Y_N, rep % Y_N

    def at_y(d):
        return (z * Y_N + (y + d + Y_N) % Y_N, dat)

    def at_z(d):
        return ((z + d) % Z_N * Y_N + y, dat)

    def at_x(d):
        return (rep, (x + d) % X_N * 2 + c)

    up, down = at_y(1), at_y(-1)

    def load(from_ref, to_ref, idx):
        return pltpu.make_async_copy(from_ref, to_ref, ld_sem.at[idx])

    own = pl.ds(0, rows)
    swp = pl.ds(rows, rows)

    @pl.when(kind == 0)
    def _():
        load(txt_ref, xk, 0).start()
        load(img_ref, xq.at[own], 1).start()
        load(wi_ref, wq, 2).start()
        load(wt_ref, wk, 3).start()

    @pl.when(kind == 1)
    def _():
        load(img_ref, xk, 0).start()
        load(txt_ref, xq.at[own], 1).start()
        load(wt_ref, wq, 2).start()
        load(wi_ref, wk, 3).start()

    greet([partner] + [at_y(d) for d in range(1, Y_N)] + [at_z(d) for d in range(1, Z_N)] + [at_x(d) for d in range(1, X_N)])
    load(txt_ref, xk, 0).wait()
    swap_copy = remote(xk, xq.at[swp], xs_sem, xr_sem, dst)
    swap_copy.start()

    def direct(g):
        return kbuf.at[g, pl.ds(0, tile)]

    def passed(g):
        return kbuf.at[g, pl.ds(tile, tile)]

    def erows(base, t):
        return eq.at[pl.ds(pl.multiple_of(base + t * tile, tile), tile)]

    def own_to_src(t):
        return remote(erows(0, t), direct(3 + t), es_sem.at[t], er_sem.at[t], src)

    def own_to_dst(t):
        return remote(erows(0, t), direct(6 + t), es_sem.at[3 + t], er_sem.at[3 + t], dst)

    def swp_to_dst(t):
        return remote(erows(rows, t), direct(9 + t), es_sem.at[6 + t], er_sem.at[6 + t], dst)

    def got_direct(g):
        remote(direct(g), direct(g), es_sem.at[0], er_sem.at[g - 3], partner).wait_recv()

    def pass_own(t):
        return remote(direct(t), passed(t), ps_sem.at[t], pr_sem.at[t], partner)

    def pass_on(g):
        return remote(direct(g), passed(g + 1), ps_sem.at[g], pr_sem.at[g], partner)

    def got_passed(i):
        remote(passed(0), passed(0), ps_sem.at[i], pr_sem.at[i], partner).wait_recv()

    def project_q(base, t):
        at = pl.ds(pl.multiple_of(base + t * tile, tile), tile)
        raw = jnp.dot(xq[at], wq[...], preferred_element_type=F32)
        inv_norm = lax.rsqrt(jnp.sum(raw * raw, axis=1, keepdims=True))
        val = raw * inv_norm
        unit[at] = val
        eq[at] = val.astype(BF16)
        inv[at] = jnp.broadcast_to(inv_norm, (tile, 128))

    def project_k(t):
        at = pl.ds(pl.multiple_of(t * tile, tile), tile)
        raw = jnp.dot(xk[at], wk[...], preferred_element_type=F32)
        inv_norm = lax.rsqrt(jnp.sum(raw * raw, axis=1, keepdims=True))
        kbuf[t, :tile] = (raw * inv_norm).astype(BF16)

    load(wt_ref, wk, 3).wait()

    def k_step(t, carry):
        project_k(t)

        @pl.when(t > 0)
        def _():
            pass_own(t - 1).start()

        return carry

    lax.fori_loop(0, 3, k_step, 0)
    load(img_ref, xq.at[own], 1).wait()
    load(wi_ref, wq, 2).wait()

    def own_step(t, carry):
        project_q(0, t)

        @pl.when(t == 0)
        def _():
            pass_own(2).start()

        return carry

    lax.fori_loop(0, 3, own_step, 0)
    acc[...] = jnp.zeros_like(acc)
    sums[...] = jnp.zeros_like(sums)

    def weigh(s_ref, h_ref, j, diag_off):
        loss, temp, tilt, lift = None, None, None, None
        for r in range(0, qt, 32):
            dots = s_ref[r : r + 32, slice(j * tile, (j + 1) * tile)]
            logit = dots * scale2 + bias2
            if diag_off is not None:
                row_ids = lax.broadcasted_iota(jnp.int32, dots.shape, 0) + (diag_off + r)
                hit = row_ids == lax.broadcasted_iota(jnp.int32, dots.shape, 1)
                logit = jnp.where(hit, -logit, logit)
            exps = jnp.exp2(jnp.minimum(logit, -logit))
            grad = jnp.exp2(jnp.minimum(logit, 0.0)) * (1.0 / (1.0 + exps))
            if diag_off is not None:
                grad = jnp.where(hit, -grad, grad)
            h_ref[r : r + 32, j * tile : (j + 1) * tile] = (grad * h_scale).astype(BF16)
            parts = [exps[i : i + 8] for i in range(0, 32, 8)]
            while len(parts) > 1:
                parts = [a + b + a * b for a, b in zip(parts[::2], parts[1::2])]
            one, two, three = fold_sum(grad * dots), fold_sum(grad), fold_sum(jnp.maximum(logit, 0.0))
            if r:
                loss = loss + parts[0] + loss * parts[0]
                temp, tilt, lift = temp + one, tilt + two, lift + three
            else:
                loss, temp, tilt, lift = parts[0], one, two, three
        sums[0] += jnp.log1p(loss)
        sums[1] += temp
        sums[2] += tilt
        sums[3] += lift

    def attend(q0, tiles, g, k0, blocks, diag_from, key_tile):
        depth = blocks * tile
        pending = []
        mid = dim // 2

        def gradient(t, n):
            at = slice(q0 + t * qt, q0 + (t + 1) * qt)
            cols = slice(n * mid, (n + 1) * mid)
            acc[at, cols] += jnp.dot(hblk[t % 2][:, :depth], kbuf[g, k0 : k0 + depth, cols], preferred_element_type=F32)

        for t in range(tiles + 1):
            if t < tiles:
                ques = eq[q0 + t * qt : q0 + (t + 1) * qt, :]
                sblk[t % 2][:, :depth] = lax.dot_general(ques, kbuf[g, k0 : k0 + depth, :], (((1,), (1,)), ((), ())), preferred_element_type=F32)
            for item in pending:
                gradient(*item)
            pending = []
            if t:
                for j in range(blocks):
                    diag = diag_from is not None and t - 1 >= diag_from and j == 0
                    weigh(sblk[(t - 1) % 2], hblk[(t - 1) % 2], j, (t - 1 - diag_from) * qt - key_tile * tile if diag else None)
                pending = [(t - 1, 0), (t - 1, 1)]
        for item in pending:
            gradient(*item)

    def first_step(t, carry):
        got_passed(t)
        attend(0, 2, t, 0, 2, 0, t)
        return carry

    lax.fori_loop(0, 3, first_step, 0)

    swap_copy.wait_send()
    for t in range(3):
        own_to_src(t).start()
    swap_copy.wait_recv()

    def swp_step(t, carry):
        project_q(rows, t)
        return carry

    lax.fori_loop(0, 3, swp_step, 0)

    def second_step(t, carry):
        @pl.when(t == 2)
        def _():
            for i in range(3):
                own_to_dst(i).start()
            for i in range(3):
                swp_to_dst(i).start()
            got_direct(3)
            pass_on(3).start()

        attend(rows, 2, t, 0, 2, None, None)
        return carry

    lax.fori_loop(0, 3, second_step, 0)
    attend(0, 4, 3, 0, 1, None, None)

    def main_step(g, carry):
        got_direct(g)
        pass_on(g).start()
        got_passed(g - 1)
        twin = (g >= 6) & (g < 9)

        @pl.when(twin)
        def _():
            attend(0, 4, g, 0, 2, 2, g - 6)

        @pl.when(jnp.logical_not(twin))
        def _():
            attend(0, 4, g, 0, 2, None, None)

        return carry

    lax.fori_loop(4, 12, main_step, 0)
    got_passed(11)
    attend(0, 4, 12, tile, 1, None, None)

    for t in range(3):
        own_to_src(t).wait_send()
        own_to_dst(t).wait_send()
        swp_to_dst(t).wait_send()

    def back_step(t, carry):
        at = pl.ds(pl.multiple_of(t * tile, tile), tile)
        grad, val = acc[at], unit[at]
        proj = jnp.sum(val * grad, axis=1, keepdims=True)
        eq[at] = (inv[at][:, :1] * (grad - val * proj)).astype(BF16)
        return carry

    lax.fori_loop(0, 6, back_step, 0)

    strip = dim // 8
    hrows = dim // 2

    def head(row0, n):
        cols = pl.ds(pl.multiple_of(row0, strip), n)
        return lax.dot_general(xq[:, cols], eq[...], (((0,), (0,)), ((), ())), preferred_element_type=F32)

    def give(t):
        at = pl.ds(pl.multiple_of(t * 2 * strip, strip), 2 * strip)
        return remote(away.at[at], landed.at[at], hs_sem.at[t], hr_sem.at[t], partner)

    def away_step(t, carry):
        away[pl.ds(pl.multiple_of(t * 2 * strip, strip), 2 * strip), :] = head((1 - c) * hrows + t * 2 * strip, 2 * strip)

        @pl.when(t == 1)
        def _():
            give(0).start()

        return carry

    lax.fori_loop(0, 2, away_step, 0)
    give(1).start()

    def home_step(t, carry):
        at = pl.ds(pl.multiple_of(t * 2 * strip, strip), 2 * strip)
        half[at, :] = head(c * hrows + t * 2 * strip, 2 * strip)
        return carry

    lax.fori_loop(0, 2, home_step, 0)
    give(0).wait_recv()
    give(1).wait_recv()

    def join_step(t, carry):
        at = pl.ds(pl.multiple_of(t * strip, strip), strip)
        half[at, :] += landed[at, :]
        return carry

    lax.fori_loop(0, 4, join_step, 0)
    lane = jnp.sum(sums[...], axis=1)
    lane = lane[:, :128] + lane[:, 128:]
    loss = lane[:1] + lane[3:] * F32(0.6931471805599453)
    sc_c[c] = jnp.concatenate([loss, lane[1:3], jnp.zeros((5, 128), F32)], axis=0)
    for t in range(2):
        give(t).wait_send()
    for t in range(3):
        pass_own(t).wait_send()
    for g in range(3, 12):
        pass_on(g).wait_send()

    hr = n // 2
    ra, rb = hr // Y_N, hr // Z_N
    rf = hr // (Y_N * Z_N)
    hh = ra // 2
    col_a, col_b = pl.ds(0, cut), pl.ds(cut, n - cut)

    def rows(start, size):
        return pl.ds(pl.multiple_of(start, 8), size)

    def pair(sem, i, src, dst_ref, peer):
        return remote(src, dst_ref, sem.at[0, i], sem.at[1, i], peer)

    sends = []

    def launch(copy):
        copy.start()
        sends.append(copy)

    def block_y(d, part_rows=None):
        first, size = part_rows or (0, ra)
        return rows((y + d + Y_N) % Y_N * ra + first, size)

    low, high = (0, hh), (hh, hh)

    wide = cut // 2
    cols = [pl.ds(h * wide, wide) for h in range(2)]
    span = [slice(h * wide, (h + 1) * wide) for h in range(2)]
    low_in = [pair(l_sem, h, half.at[block_y(2, low), cols[h]], ylow.at[:, cols[h]], up) for h in range(2)]
    high_in = [pair(l_sem, 2 + h, half.at[block_y(2, high), cols[h]], yhigh.at[:, cols[h]], down) for h in range(2)]
    own_up = [pair(k_sem, h, half.at[block_y(1, high), cols[h]], yring.at[0, pl.ds(hh, hh), cols[h]], up) for h in range(2)]
    own_down = [pair(k_sem, 2 + h, half.at[block_y(-1, low), cols[h]], yring.at[1, pl.ds(0, hh), cols[h]], down) for h in range(2)]
    sum_up = [pair(k_sem, 4 + h, ylow.at[:, cols[h]], yring.at[0, pl.ds(0, hh), cols[h]], up) for h in range(2)]
    sum_down = [pair(k_sem, 6 + h, yhigh.at[:, cols[h]], yring.at[1, pl.ds(hh, hh), cols[h]], down) for h in range(2)]
    b_copies = [pair(b_sem, d - 1, half.at[rows((z + d) % Z_N * rb, rb), col_b], bufb.at[d - 1], at_z(d)) for d in range(1, Z_N)]
    for copy in low_in + high_in + b_copies + own_up + own_down:
        launch(copy)
    cc = pair(c_sem, 0, sc_c.at[c], sc_c.at[c], partner)
    launch(cc)
    for h in range(2):
        low_in[h].wait_recv()
        ylow[:, span[h]] += half[block_y(1, low), span[h]]
        high_in[h].wait_recv()
        launch(sum_up[h])
        yhigh[:, span[h]] += half[block_y(-1, high), span[h]]
        launch(sum_down[h])
    cc.wait_recv()
    sc_y[y] = sc_c[0] + sc_c[1]
    y_copies = [pair(c_sem, d, sc_y.at[y], sc_y.at[y], at_y(d)) for d in range(1, Y_N)]
    for copy in y_copies:
        launch(copy)

    def straight(h, d):
        i = h * (Z_N - 1) + d - 1
        return pair(a2_sem, i, ysum.at[rows((z + d) % Z_N * rf, rf), cols[h]], bufa2.at[d - 1, :, cols[h]], at_z(d))

    for copy in b_copies:
        copy.wait_recv()
    tot = half[rows(z * rb, rb), cut:n]
    for d in range(1, Z_N):
        tot = tot + bufb[d - 1]
    zsum[...] = tot
    a2_copies = [[straight(h, d) for d in range(1, Z_N)] for h in range(2)]
    for h in range(2):
        for copies in (own_up, own_down, sum_up, sum_down):
            copies[h].wait_recv()
        ysum[:, span[h]] = (half[block_y(0), span[h]] + yring[0, :, span[h]]) + yring[1, :, span[h]]
        for copy in a2_copies[h]:
            launch(copy)
    b2_copies = [pair(b2_sem, d - 1, zsum.at[rows((y + d) % Y_N * rf, rf)], bufb2.at[d - 1], at_y(d)) for d in range(1, Y_N)]
    for copy in b2_copies:
        launch(copy)

    for copy in y_copies:
        copy.wait_recv()
    tot = sc_y[0]
    for i in range(1, Y_N):
        tot = tot + sc_y[i]
    sc_z[z] = tot
    z_copies = [pair(c_sem, Y_N + d, sc_z.at[z], sc_z.at[z], at_z(d)) for d in range(1, Z_N)]
    for copy in z_copies:
        launch(copy)

    x_cols = [cols[0], pl.ds(wide, n - wide)]
    x_copies = [pair(x_sem, h, part.at[:, x_cols[h]], bufx.at[0, :, x_cols[h]], at_x(2)) for h in range(2)]
    for h in range(2):
        for copy in a2_copies[h]:
            copy.wait_recv()
        tot = ysum[rows(z * rf, rf), span[h]]
        for d in range(1, Z_N):
            tot = tot + bufa2[d - 1, :, span[h]]
        part[:, span[h]] = tot
        if h:
            for copy in b2_copies:
                copy.wait_recv()
            tot = zsum[rows(y * rf, rf), :]
            for d in range(1, Y_N):
                tot = tot + bufb2[d - 1]
            part[:, cut:n] = tot
        launch(x_copies[h])

    for copy in z_copies:
        copy.wait_recv()
    tot = sc_z[0]
    for i in range(1, Z_N):
        tot = tot + sc_z[i]
    sc_x[x] = tot
    s_copies = [pair(c_sem, Y_N + Z_N + d, sc_x.at[x], sc_x.at[x], at_x(d)) for d in range(1, X_N)]
    for copy in s_copies:
        launch(copy)

    base = c * hr
    fin_a = rows(base + y * ra + z * rf, rf)
    fin_b = rows(base + z * rb + y * rf, rf)

    def by_kind(act):
        @pl.when(kind == 0)
        def _():
            act(img_out, txt_out)

        @pl.when(kind == 1)
        def _():
            act(txt_out, img_out)

    def same(sem, i, ref, at, peer):
        return pair(sem, i, ref.at[at], ref.at[at], peer)

    def put(mine, i):
        at, col = (fin_b, col_b) if i == 2 else (fin_a, cols[i])
        return pltpu.make_async_copy(bufx.at[1, :, col], mine.at[at, col], fin_sem.at[i])

    def gather_b(mine, d):
        return pair(gb_sem, d - 1, bufx.at[1, :, col_b], mine.at[fin_b, col_b], at_y(d))

    def gather_a(mine, h, d):
        return pair(ga_sem, h * (Z_N - 1) + d - 1, bufx.at[1, :, cols[h]], mine.at[fin_a, cols[h]], at_z(d))

    def start_a(mine, other, h):
        for d in range(1, Z_N):
            gather_a(mine, h, d).start()
        put(mine, h).start()

    def start_b(mine, other):
        for d in range(1, Y_N):
            gather_b(mine, d).start()
        put(mine, 2).start()

    x_copies[0].wait_recv()
    bufx[1, :, span[0]] = part[:, span[0]] + bufx[0, :, span[0]]
    by_kind(lambda mine, other: start_a(mine, other, 0))
    x_copies[1].wait_recv()
    bufx[1, :, wide:n] = part[:, wide:n] + bufx[0, :, wide:n]
    by_kind(start_b)
    by_kind(lambda mine, other: start_a(mine, other, 1))
    for copy in s_copies:
        copy.wait_recv()
    tot = sc_x[0]
    for i in range(1, X_N):
        tot = tot + sc_x[i]
    tot = tot * (F32(0.5) * inv_n)
    loss_out[0, 0] = jnp.sum(tot[0:1])
    temp_out[0, 0] = jnp.sum(tot[1:2] * temp[:, :128])
    bias_out[0, 0] = jnp.sum(tot[2:3])
    for i in range(3):
        put(img_out, i).wait()

    first_z = 2 * Y_N

    def piece(i, core):
        if i < first_z:
            return (rows(core * hr + (y - i // 2 + Y_N) % Y_N * ra, ra), cols[i % 2])
        return (rows(core * hr + (z - i + first_z + Z_N) % Z_N * rb, rb), col_b)

    def quarter(d, part_rows, h):
        return (rows(base + (y + d + Y_N) % Y_N * ra + part_rows[0], part_rows[1]), cols[h])

    def forward(mine, i):
        return pair(f_sem, i, mine.at[piece(i, c)], mine.at[piece(i, c)], dst)

    def spread(mine, other, i):
        forward(mine, i).start()
        same(m_sem, i, mine, piece(i, c), partner).start()

    def over_z(mine, d):
        return same(hb_sem, d - 1, mine, piece(first_z, c), at_z(d))

    def full(mine, i, h):
        return same(ha_sem, 2 * h + i, mine, piece(h, c), up if i == 0 else down)

    def onward(mine, i, h):
        return same(ha_sem, 4 + 2 * h + i, mine, quarter(-1, low, h) if i == 0 else quarter(1, high, h), up if i == 0 else down)

    arrived = []

    def second_a(h):
        for d in range(1, Z_N):
            gather_a(img_out, h, d).wait_recv()

        def act(mine, other):
            full(mine, 0, h).start()
            full(mine, 1, h).start()
            spread(mine, other, h)

        by_kind(act)
        arrived.append(h)

    def second_b(mine, other):
        for d in range(1, Z_N):
            over_z(mine, d).start()
        spread(mine, other, first_z)

    def z_pieces(ds):
        for d in ds:
            same(hb_sem, d - 1, img_out, piece(first_z + d, c), partner).wait_recv()
            arrived.append(first_z + d)

        def act(mine, other):
            for d in ds:
                spread(mine, other, first_z + d)

        by_kind(act)

    def third_a(h):
        for i in range(2):
            full(img_out, i, h).wait_recv()

        def act(mine, other):
            onward(mine, 0, h).start()
            onward(mine, 1, h).start()
            spread(mine, other, 2 + h)
            spread(mine, other, 6 + h)

        by_kind(act)
        arrived.extend([2 + h, 6 + h])

    def fourth_a(h):
        for i in range(2):
            onward(img_out, i, h).wait_recv()
        by_kind(lambda mine, other: spread(mine, other, 4 + h))
        arrived.append(4 + h)

    second_a(0)
    for d in range(1, Y_N):
        gather_b(img_out, d).wait_recv()
    by_kind(second_b)
    arrived.append(first_z)
    second_a(1)
    third_a(0)
    z_pieces([1, Z_N - 1])
    third_a(1)
    z_pieces([2, Z_N - 2])
    fourth_a(0)
    z_pieces([3, Z_N - 3])
    fourth_a(1)
    z_pieces(list(range(4, Z_N - 3)))

    def across(group):
        for i in group:
            forward(img_out, i).wait_recv()

        def act(mine, other):
            for i in group:
                same(o_sem, i, other, piece(i, c), partner).start()

        by_kind(act)

    for at in range(0, len(arrived), 2):
        across(arrived[at : at + 2])
    for i in arrived:
        same(m_sem, i, img_out, piece(i, 1 - c), partner).wait_recv()
    for i in arrived:
        same(o_sem, i, img_out, piece(i, 1 - c), partner).wait_recv()
    for copy in sends:
        copy.wait_send()
    for d in range(1, Y_N):
        gather_b(img_out, d).wait_send()
    for d in range(1, Z_N):
        over_z(img_out, d).wait_send()
        for h in range(2):
            gather_a(img_out, h, d).wait_send()
    for h in range(2):
        for i in range(2):
            full(img_out, i, h).wait_send()
            onward(img_out, i, h).wait_send()
    for i in arrived:
        forward(img_out, i).wait_send()
        same(m_sem, i, img_out, piece(i, c), partner).wait_send()
        same(o_sem, i, img_out, piece(i, c), partner).wait_send()


def place_kernel(img_in, txt_in, img_out, txt_out, stage, in_sem, out_sem):
    parts, size, _ = stage.shape

    def copies(i):
        from_ref, to_ref = (img_in, img_out) if i < parts // 2 else (txt_in, txt_out)
        at = pl.ds(i % (parts // 2) * size, size)
        return (
            pltpu.make_async_copy(from_ref.at[at], stage.at[i], in_sem.at[i]),
            pltpu.make_async_copy(stage.at[i], to_ref.at[at], out_sem.at[i]),
        )

    for i in range(parts):
        copies(i)[0].start()
    for i in range(parts):
        come, go = copies(i)
        come.wait()
        go.start()
    for i in range(parts):
        copies(i)[1].wait()


def pair_sems(count):
    return pltpu.SemaphoreType.DMA((2, count))


def head_gradients(img_loc, txt_loc, w_img, w_txt, log_temp, logit_bias, total_rows):
    rows, dim = img_loc.shape
    any_spec = pl.BlockSpec(memory_space=pl.ANY)
    smem_spec = pl.BlockSpec(memory_space=pltpu.SMEM)
    tile, qt = rows // 3, rows // 2
    dma = pltpu.SemaphoreType.DMA
    flops = 2 * rows * dim * dim * 7 + 4 * 2 * rows * 8 * rows * dim
    cut = (dim * 3 // 4) // 128 * 128
    hr = dim // 2
    ra, rb, rf = hr // Y_N, hr // Z_N, hr // (Y_N * Z_N)
    nb = dim - cut
    head = jax.ShapeDtypeStruct((dim, dim), F32)
    vmem = pltpu.VMEM
    dw_img, dw_txt, loss, d_temp, d_bias = pl.pallas_call(
        functools.partial(whole_kernel, total_rows, rows, dim, cut),
        out_shape=(head, head) + (jax.ShapeDtypeStruct((1, 1), F32),) * 3,
        in_specs=[smem_spec] * 2 + [any_spec] * 4,
        out_specs=(any_spec, any_spec, smem_spec, smem_spec, smem_spec),
        scratch_shapes=[
            vmem((2 * rows, dim), BF16),
            vmem((rows, dim), BF16),
            vmem((dim, dim), BF16),
            vmem((dim, dim), BF16),
            vmem((13, 2 * tile, dim), BF16),
            vmem((2 * rows, dim), BF16),
            vmem((2 * rows, dim), F32),
            vmem((2 * rows, 128), F32),
            vmem((2 * rows, dim), F32),
            vmem((qt, 2 * tile), F32),
            vmem((qt, 2 * tile), F32),
            vmem((qt, 2 * tile), BF16),
            vmem((qt, 2 * tile), BF16),
            vmem((4, 8, tile), F32),
            vmem((hr, dim), F32),
            vmem((hr, dim), F32),
            vmem((hr, dim), F32),
            vmem((ra, cut), F32),
            vmem((rb, nb), F32),
            vmem((ra // 2, cut), F32),
            vmem((ra // 2, cut), F32),
            vmem((2, ra, cut), F32),
            vmem((Z_N - 1, rb, nb), F32),
            vmem((Z_N - 1, rf, cut), F32),
            vmem((Y_N - 1, rf, nb), F32),
            vmem((rf, dim), F32),
            vmem((2, rf, dim), F32),
            vmem((C_N, 8, 128), F32),
            vmem((Y_N, 8, 128), F32),
            vmem((Z_N, 8, 128), F32),
            vmem((X_N, 8, 128), F32),
            dma((4,)), dma, dma, dma((9,)), dma((9,)), dma((12,)), dma((12,)), dma((2,)), dma((2,)),
            pair_sems(4), pair_sems(8), pair_sems(Z_N - 1), pair_sems(2 * (Z_N - 1)), pair_sems(Y_N - 1),
            pair_sems(2), pair_sems(X_N + Y_N + Z_N), pair_sems(2 * (Z_N - 1)), pair_sems(8), pair_sems(Y_N - 1),
            pair_sems(Z_N - 1), pair_sems(2 * Y_N + Z_N), pair_sems(2 * Y_N + Z_N), pair_sems(2 * Y_N + Z_N), dma((3,)),
        ],
        compiler_params=pltpu.CompilerParams(collective_id=0, has_side_effects=True, vmem_limit_bytes=VMEM_CAP),
        cost_estimate=pl.CostEstimate(flops=flops, bytes_accessed=16 << 20, transcendentals=0),
        name="contrast",
    )(log_temp.reshape(1), logit_bias.reshape(1), img_loc, txt_loc, w_img, w_txt)
    dw_img, dw_txt = pl.pallas_call(
        place_kernel,
        out_shape=(head, head),
        in_specs=[any_spec, any_spec],
        out_specs=(any_spec, any_spec),
        scratch_shapes=[vmem((8, dim // 4, dim), F32), dma((8,)), dma((8,))],
        compiler_params=pltpu.CompilerParams(vmem_limit_bytes=VMEM_CAP),
        name="place",
    )(dw_img, dw_txt)
    return loss.reshape(()), d_temp.reshape(()), d_bias.reshape(()), dw_img, dw_txt


def solution(mesh):
    devices = mesh.shape["rep"] * mesh.shape["data"]
    row_spec = P(("rep", "data"), None)

    def device_body(img_loc, txt_loc, w_img, w_txt, log_temp, logit_bias):
        return head_gradients(img_loc, txt_loc, w_img, w_txt, log_temp, logit_bias, img_loc.shape[0] * devices)

    return jax.shard_map(device_body, mesh=mesh, in_specs=(row_spec, row_spec, P(), P(), P(), P()), out_specs=(P(), P(), P(), P(), P()), check_vma=False)
```
